8 devices in a mesh: fsdp: 4 (over z, y, x), model: 2 (over core).
Axes of the slice: x: 2, y: 2, z: 1, core: 2. Of those that a mesh axis runs over, the one named last changes fastest.
Arguments:
- x_in: bfloat16 [16, 1024, 1536], P('fsdp', 'model')
- grad_out: bfloat16 [16, 1024, 1536], P('fsdp', 'model')
- gain_attn: float32 [1536], replicated
- gain_mlp: float32 [1536], replicated
- w_qkv: bfloat16 [1536, 2048], P('fsdp', 'model')
- w_out: bfloat16 [1536, 1536], P('model', 'fsdp')
- w_gate: bfloat16 [1536, 8960], P('fsdp', 'model')
- w_up: bfloat16 [1536, 8960], P('fsdp', 'model')
- w_down: bfloat16 [8960, 1536], P('model', 'fsdp')
- rope_cos: float32 [1024, 64], replicated
- rope_sin: float32 [1024, 64], replicated
Outputs:
- output 1: bfloat16 [16, 1024, 1536], P('fsdp', 'model')
- output 2: bfloat16 [16, 1024, 1536], P('fsdp', 'model')
- output 3: float32 [1536], replicated
- output 4: float32 [1536], replicated
- output 5: float32 [1536, 2048], P('fsdp', 'model')
- output 6: float32 [1536, 1536], P('model', 'fsdp')
- output 7: float32 [1536, 8960], P('fsdp', 'model')
- output 8: float32 [1536, 8960], P('fsdp', 'model')
- output 9: float32 [8960, 1536], P('model', 'fsdp')
All inputs are finite; a program needn't handle non-finite values.
Results may differ from the reference program's by a relative error of at most 0.0157642.
Values are sent between devices in bfloat16 or wider.
A program may use at most 1 GiB of HBM per device.

```python
import jax
import jax.numpy as jnp
from jax import lax

BATCH = 16
SEQ_LEN = 1024
D_MODEL = 1536
D_FF = 8960
HEADS = 12
KV_HEADS = 2
HEAD_DIM = 128
GROUP_SIZE = HEADS // KV_HEADS
QKV_COLS = KV_HEADS * (GROUP_SIZE + 2) * HEAD_DIM
NORM_EPS = 1e-5
ROPE_BASE = 500000.0


def rope_tables(key):
    step_key, offset_key = jax.random.split(key)
    steps = jax.random.randint(step_key, (SEQ_LEN,), 1, 4)
    offset = jax.random.randint(offset_key, (), 0, 1024)
    positions = (jnp.cumsum(steps) + offset).astype(jnp.float32)
    freqs = ROPE_BASE ** (-jnp.arange(0, HEAD_DIM, 2).astype(jnp.float32) / HEAD_DIM)
    angles = positions[:, None] * freqs[None, :]
    return jnp.cos(angles), jnp.sin(angles)


def normal_weight(key, rows, cols):
    return (jax.random.normal(key, (rows, cols), jnp.float32) * rows ** -0.5).astype(jnp.bfloat16)


def setup_inputs(seed: int = 0) -> dict:
    keys = jax.random.split(jax.random.key(seed), 10)
    act_shape = (BATCH, SEQ_LEN, D_MODEL)
    rope_cos, rope_sin = rope_tables(keys[9])
    return {
        'x_in': jax.random.normal(keys[0], act_shape, jnp.float32).astype(jnp.bfloat16),
        'grad_out': jax.random.normal(keys[1], act_shape, jnp.float32).astype(jnp.bfloat16),
        'gain_attn': 1.0 + 0.3 * jax.random.normal(keys[2], (D_MODEL,), jnp.float32),
        'gain_mlp': 1.0 + 0.3 * jax.random.normal(keys[3], (D_MODEL,), jnp.float32),
        'w_qkv': normal_weight(keys[4], D_MODEL, QKV_COLS),
        'w_out': normal_weight(keys[5], HEADS * HEAD_DIM, D_MODEL),
        'w_gate': normal_weight(keys[6], D_MODEL, D_FF),
        'w_up': normal_weight(keys[7], D_MODEL, D_FF),
        'w_down': normal_weight(keys[8], D_FF, D_MODEL),
        'rope_cos': rope_cos,
        'rope_sin': rope_sin,
    }


def rms_norm(x_f32, gain):
    inv_rms = lax.rsqrt(jnp.mean(x_f32 * x_f32, axis=-1, keepdims=True) + NORM_EPS)
    return (x_f32 * inv_rms * gain).astype(jnp.bfloat16)


def rotate(tensor, cos_t, sin_t):
    half = HEAD_DIM // 2
    first = tensor[..., :half]
    second = tensor[..., half:]
    return jnp.concatenate([first * cos_t - second * sin_t, second * cos_t + first * sin_t], axis=-1)


def matmul(left, right):
    return jnp.dot(left.astype(jnp.float32), right.astype(jnp.float32))


def layer_seq(x_seq, params, rope_cos, rope_sin):
    gain_attn, gain_mlp, w_qkv, w_out, w_gate, w_up, w_down = params
    x_f32 = x_seq.astype(jnp.float32)
    h_attn = rms_norm(x_f32, gain_attn)
    qkv = matmul(h_attn, w_qkv).reshape(SEQ_LEN, KV_HEADS, GROUP_SIZE + 2, HEAD_DIM)
    query = rotate(qkv[:, :, :GROUP_SIZE], rope_cos[:, None, None, :], rope_sin[:, None, None, :]).astype(jnp.bfloat16)
    key_rot = rotate(qkv[:, :, GROUP_SIZE], rope_cos[:, None, :], rope_sin[:, None, :]).astype(jnp.bfloat16)
    value = qkv[:, :, GROUP_SIZE + 1].astype(jnp.bfloat16)
    scores = jnp.einsum('qkgd,tkd->kgqt', query.astype(jnp.float32), key_rot.astype(jnp.float32)) * HEAD_DIM ** -0.5
    pos_ids = jnp.arange(SEQ_LEN)
    scores = jnp.where(pos_ids[:, None] >= pos_ids[None, :], scores, -1e30)
    attn_prob = jax.nn.softmax(scores, axis=-1).astype(jnp.bfloat16)
    attn = jnp.einsum('kgqt,tkd->qkgd', attn_prob.astype(jnp.float32), value.astype(jnp.float32)).astype(jnp.bfloat16)
    attn_proj = matmul(attn.reshape(SEQ_LEN, HEADS * HEAD_DIM), w_out).astype(jnp.bfloat16)
    mid_f32 = (x_f32 + attn_proj.astype(jnp.float32)).astype(jnp.bfloat16).astype(jnp.float32)
    h_mlp = rms_norm(mid_f32, gain_mlp)
    gate = matmul(h_mlp, w_gate)
    up_proj = matmul(h_mlp, w_up)
    gated_act = (jax.nn.silu(gate) * up_proj).astype(jnp.bfloat16)
    mlp_out = matmul(gated_act, w_down).astype(jnp.bfloat16)
    return (mid_f32 + mlp_out.astype(jnp.float32)).astype(jnp.bfloat16)


def reference(x_in, grad_out, gain_attn, gain_mlp, w_qkv, w_out, w_gate, w_up, w_down, rope_cos, rope_sin):
    params = tuple(weight.astype(jnp.float32) for weight in (gain_attn, gain_mlp, w_qkv, w_out, w_gate, w_up, w_down))

    def layer_fn(x_seq, param_set):
        return layer_seq(x_seq, param_set, rope_cos, rope_sin)

    def seq_step(accum, seq_pair):
        x_seq, dy_seq = seq_pair
        y_seq, vjp_fn = jax.vjp(layer_fn, x_seq, params)
        dx_seq, dparams = vjp_fn(dy_seq)
        return jax.tree.map(jnp.add, accum, dparams), (y_seq, dx_seq)

    zero_grads = jax.tree.map(jnp.zeros_like, params)
    grads, (y_out, dx_in) = lax.scan(seq_step, zero_grads, (x_in, grad_out))
    return (y_out, dx_in, grads[0], grads[1], grads[2], grads[3], grads[4], grads[5], grads[6])
```

```python
import functools

import jax
import jax.numpy as jnp
from jax import lax
from jax.experimental import pallas as pl
from jax.experimental.pallas import tpu as pltpu
from jax.sharding import PartitionSpec as P


NORM_EPS = 1e-5
NEG = -1e30
QB = 256


def rms_scale(x_f32, gain):
    inv_rms = lax.rsqrt(jnp.mean(x_f32 * x_f32, axis=-1, keepdims=True) + NORM_EPS)
    return x_f32 * inv_rms * gain


def nt(a, b):
    return lax.dot_general(a, b, (((1,), (1,)), ((), ())), preferred_element_type=jnp.float32)


def nn(a, b):
    return lax.dot_general(a, b, (((1,), (0,)), ((), ())), preferred_element_type=jnp.float32)


def tn(a, b):
    return lax.dot_general(a, b, (((0,), (0,)), ((), ())), preferred_element_type=jnp.float32)


def causal_mask():
    rows = lax.broadcasted_iota(jnp.int32, (QB, QB), 0)
    cols = lax.broadcasted_iota(jnp.int32, (QB, QB), 1)
    return rows >= cols


def softmax_chunks(q, k_ref, blk, scale, mask):
    lo = blk * QB
    s_diag = jnp.where(mask, nt(q, k_ref[lo:lo + QB, :]) * scale, NEG)
    top = jnp.max(s_diag, axis=-1, keepdims=True)
    if blk:
        s_off = nt(q, k_ref[:lo, :]) * scale
        top = jnp.maximum(top, jnp.max(s_off, axis=-1, keepdims=True))
        e_off = jnp.exp(s_off - top)
        e_diag = jnp.exp(s_diag - top)
        inv = 1.0 / (jnp.sum(e_off, axis=-1, keepdims=True) + jnp.sum(e_diag, axis=-1, keepdims=True))
        return e_off * inv, e_diag * inv
    e_diag = jnp.exp(s_diag - top)
    return None, e_diag * (1.0 / jnp.sum(e_diag, axis=-1, keepdims=True))


def attn_fwd_kernel(heads, seq, dim, idx_ref, qkv_ref, cos_ref, sin_ref, rot_ref, out_ref, k_scr, v_scr):
    half_rows = seq // 2
    first = idx_ref[0]
    where_half = (first, 1 - first)
    mask = causal_mask()
    scale = dim ** -0.5
    kcol, vcol = heads * dim, (heads + 1) * dim
    for half in range(2):
        st = where_half[half]
        rows = slice(half * half_rows, (half + 1) * half_rows)
        key = qkv_ref[st, 0, :, kcol:kcol + dim]
        key = (key * cos_ref[st] + pltpu.roll(key, dim // 2, 1) * sin_ref[st]).astype(jnp.bfloat16)
        val = qkv_ref[st, 0, :, vcol:vcol + dim].astype(jnp.bfloat16)
        k_scr[rows, :] = key
        v_scr[rows, :] = val
        rot_ref[st, 0, :, kcol:kcol + dim] = key
        rot_ref[st, 0, :, vcol:vcol + dim] = val

    @pl.loop(0, heads)
    def _(h):
        col = pl.ds(pl.multiple_of(h * dim, dim), dim)
        for blk in range(seq // QB):
            st = where_half[blk * QB // half_rows]
            r0 = blk * QB % half_rows
            rows = slice(r0, r0 + QB)
            q = qkv_ref[st, 0, rows, col]
            q = (q * cos_ref[st, rows, :] + pltpu.roll(q, dim // 2, 1) * sin_ref[st, rows, :]).astype(jnp.bfloat16)
            rot_ref[st, 0, rows, col] = q
            p_off, p_diag = softmax_chunks(q, k_scr, blk, scale, mask)
            lo = blk * QB
            o = nn(p_diag.astype(jnp.bfloat16), v_scr[lo:lo + QB, :])
            if blk:
                o = o + nn(p_off.astype(jnp.bfloat16), v_scr[:lo, :])
            out_ref[st, 0, rows, col] = o.astype(jnp.bfloat16)


def attn_bwd_kernel(heads, seq, dim, idx_ref, rot_ref, do_ref, cos_ref, sin_ref, dqkv_ref, k_scr, v_scr, dk_scr, dv_scr):
    half_rows = seq // 2
    first = idx_ref[0]
    where_half = (first, 1 - first)
    mask = causal_mask()
    scale = dim ** -0.5
    kcol, vcol = heads * dim, (heads + 1) * dim
    for half in range(2):
        st = where_half[half]
        rows = slice(half * half_rows, (half + 1) * half_rows)
        k_scr[rows, :] = rot_ref[st, 0, :, kcol:kcol + dim]
        v_scr[rows, :] = rot_ref[st, 0, :, vcol:vcol + dim]
    dk_scr[...] = jnp.zeros_like(dk_scr)
    dv_scr[...] = jnp.zeros_like(dv_scr)

    @pl.loop(0, heads)
    def _(h):
        col = pl.ds(pl.multiple_of(h * dim, dim), dim)
        for blk in range(seq // QB):
            st = where_half[blk * QB // half_rows]
            r0 = blk * QB % half_rows
            rows = slice(r0, r0 + QB)
            lo = blk * QB
            q = rot_ref[st, 0, rows, col]
            do = do_ref[st, 0, rows, col]
            p_off, p_diag = softmax_chunks(q, k_scr, blk, scale, mask)
            dp_diag = nt(do, v_scr[lo:lo + QB, :])
            row_dot = jnp.sum(dp_diag * p_diag, axis=-1, keepdims=True)
            if blk:
                dp_off = nt(do, v_scr[:lo, :])
                row_dot = row_dot + jnp.sum(dp_off * p_off, axis=-1, keepdims=True)
            ds_diag = (p_diag * (dp_diag - row_dot) * scale).astype(jnp.bfloat16)
            dq = nn(ds_diag, k_scr[lo:lo + QB, :])
            dk_scr[lo:lo + QB, :] += tn(ds_diag, q)
            dv_scr[lo:lo + QB, :] += tn(p_diag.astype(jnp.bfloat16), do)
            if blk:
                ds_off = (p_off * (dp_off - row_dot) * scale).astype(jnp.bfloat16)
                dq = dq + nn(ds_off, k_scr[:lo, :])
                dk_scr[:lo, :] += tn(ds_off, q)
                dv_scr[:lo, :] += tn(p_off.astype(jnp.bfloat16), do)
            dq = dq * cos_ref[st, rows, :] - pltpu.roll(dq, dim // 2, 1) * sin_ref[st, rows, :]
            dqkv_ref[st, 0, rows, col] = dq.astype(jnp.bfloat16)

    for half in range(2):
        st = where_half[half]
        rows = slice(half * half_rows, (half + 1) * half_rows)
        dk = dk_scr[rows, :]
        dk = dk * cos_ref[st] - pltpu.roll(dk, dim // 2, 1) * sin_ref[st]
        dqkv_ref[st, 0, :, kcol:kcol + dim] = dk.astype(jnp.bfloat16)
        dqkv_ref[st, 0, :, vcol:vcol + dim] = dv_scr[rows, :].astype(jnp.bfloat16)


def seq_block(rows, cols):
    return pl.BlockSpec((2, 1, rows, cols), lambda b, idx: (0, b, 0, 0))


def table_block(rows, dim):
    return pl.BlockSpec((2, rows, dim), lambda b, idx: (0, 0, 0))


def attn_fwd(idx, qkv, cos_t, sin_t, heads):
    _, batch, rows, cols = qkv.shape
    dim = cos_t.shape[-1]
    flops = batch * heads * rows * rows * dim * 10
    return pl.pallas_call(
        functools.partial(attn_fwd_kernel, heads, 2 * rows, dim),
        out_shape=(jax.ShapeDtypeStruct(qkv.shape, jnp.bfloat16),
                   jax.ShapeDtypeStruct((2, batch, rows, heads * dim), jnp.bfloat16)),
        grid_spec=pltpu.PrefetchScalarGridSpec(
            num_scalar_prefetch=1, grid=(batch,),
            in_specs=[seq_block(rows, cols), table_block(rows, dim), table_block(rows, dim)],
            out_specs=[seq_block(rows, cols), seq_block(rows, heads * dim)],
            scratch_shapes=[pltpu.VMEM((2 * rows, dim), jnp.bfloat16)] * 2),
        cost_estimate=pl.CostEstimate(flops=flops, bytes_accessed=qkv.size * 8, transcendentals=batch * heads * rows * rows * 2),
        compiler_params=pltpu.CompilerParams(dimension_semantics=("arbitrary",)),
        name="attn_fwd",
    )(idx, qkv, cos_t, sin_t)


def attn_bwd(idx, rot, d_attn, cos_t, sin_t, heads):
    _, batch, rows, cols = rot.shape
    dim = cos_t.shape[-1]
    flops = batch * heads * rows * rows * dim * 25
    return pl.pallas_call(
        functools.partial(attn_bwd_kernel, heads, 2 * rows, dim),
        out_shape=jax.ShapeDtypeStruct(rot.shape, jnp.bfloat16),
        grid_spec=pltpu.PrefetchScalarGridSpec(
            num_scalar_prefetch=1, grid=(batch,),
            in_specs=[seq_block(rows, cols), seq_block(rows, heads * dim), table_block(rows, dim), table_block(rows, dim)],
            out_specs=seq_block(rows, cols),
            scratch_shapes=[pltpu.VMEM((2 * rows, dim), jnp.bfloat16)] * 2 + [pltpu.VMEM((2 * rows, dim), jnp.float32)] * 2),
        cost_estimate=pl.CostEstimate(flops=flops, bytes_accessed=rot.size * 6, transcendentals=batch * heads * rows * rows * 2),
        compiler_params=pltpu.CompilerParams(dimension_semantics=("arbitrary",)),
        name="attn_bwd",
    )(idx, rot, d_attn, cos_t, sin_t)


def solution(mesh):
    act_spec = P('fsdp', 'model', None)
    rows_spec = P('fsdp', 'model')
    cols_spec = P('model', 'fsdp')
    swap = [(0, 1), (1, 0)]

    def gather_rows(w_shard):
        return lax.all_gather(w_shard, 'fsdp', axis=0, tiled=True)

    def gather_cols(w_shard):
        return lax.all_gather(w_shard, 'fsdp', axis=1, tiled=True)

    def scatter(tensor, dim):
        return lax.psum_scatter(tensor, 'fsdp', scatter_dimension=dim, tiled=True)

    def partner(tensor):
        return lax.ppermute(tensor, 'model', swap)

    def both(own):
        return jnp.stack([own, partner(own)])

    def dot(spec, left, right):
        return jnp.einsum(spec, left, right, preferred_element_type=jnp.float32)

    def device_fn(x_loc, dy_loc, gain_attn, gain_mlp, wqkv_sh, wout_sh, wgate_sh, wup_sh, wdown_sh, rope_cos, rope_sin):
        dim = 2 * rope_cos.shape[1]
        heads = wout_sh.shape[0] // dim
        half_rows = x_loc.shape[1]
        me = lax.axis_index('model')
        idx = jnp.reshape(me, (1,)).astype(jnp.int32)

        def table(first, second):
            full = jnp.concatenate([first, second], axis=-1).reshape(2, half_rows, dim)
            return jnp.where(me == 0, full, full[::-1])

        cos_t = table(rope_cos, rope_cos)
        sin_t = table(-rope_sin, rope_sin)

        w_qkv = gather_rows(wqkv_sh)
        w_out = gather_cols(wout_sh)

        x_f32 = x_loc.astype(jnp.float32)
        h_attn_f, norm_back_attn = jax.vjp(rms_scale, x_f32, gain_attn)
        h_own = h_attn_f.astype(jnp.bfloat16)
        wgate_sh, h_own = lax.optimization_barrier((wgate_sh, h_own))
        w_gate = gather_rows(wgate_sh)
        h_attn = both(h_own)
        dy = both(dy_loc)
        qkv = dot('tbsd,dc->tbsc', h_attn, w_qkv)
        wup_sh, qkv = lax.optimization_barrier((wup_sh, qkv))
        w_up = gather_rows(wup_sh)
        rot, attn = attn_fwd(idx, qkv, cos_t, sin_t, heads)
        wdown_sh, attn = lax.optimization_barrier((wdown_sh, attn))
        w_down = gather_cols(wdown_sh)
        out_other = partner(dot('bsh,hd->bsd', attn[1], w_out))
        attn_red = dot('bsh,hd->bsd', attn[0], w_out) + out_other
        mid_f32 = (x_f32 + attn_red.astype(jnp.bfloat16).astype(jnp.float32)).astype(jnp.bfloat16).astype(jnp.float32)
        h_mlp_f, norm_back_mlp = jax.vjp(rms_scale, mid_f32, gain_mlp)
        h_mlp = both(h_mlp_f.astype(jnp.bfloat16))

        gate = dot('tbsd,df->tbsf', h_mlp, w_gate)
        up_proj = dot('tbsd,df->tbsf', h_mlp, w_up)
        sig_gate = jax.nn.sigmoid(gate)
        silu_gate = gate * sig_gate
        gated_act = (silu_gate * up_proj).astype(jnp.bfloat16)
        full_down, dy = lax.optimization_barrier((dot('tbsf,tbsd->fd', gated_act, dy), dy))
        dw_down = scatter(full_down, 1)

        d_act = dot('tbsd,fd->tbsf', dy, w_down).astype(jnp.bfloat16).astype(jnp.float32)
        d_gate = (d_act * up_proj * sig_gate * (1.0 + gate * (1.0 - sig_gate))).astype(jnp.bfloat16)
        d_up = (d_act * silu_gate).astype(jnp.bfloat16)
        full_gate, h_mlp = lax.optimization_barrier((dot('tbsd,tbsf->df', h_mlp, d_gate), h_mlp))
        dw_gate = scatter(full_gate, 0)
        full_up, d_gate, d_up = lax.optimization_barrier((dot('tbsd,tbsf->df', h_mlp, d_up), d_gate, d_up))
        dw_up = scatter(full_up, 0)

        def dh_of(part):
            return (dot('bsf,df->bsd', d_gate[part], w_gate)
                    + dot('bsf,df->bsd', d_up[part], w_up))

        dh_other = partner(dh_of(1))
        dh_mlp = dh_of(0) + dh_other
        d_mid_norm, d_gain_mlp = norm_back_mlp(dh_mlp.astype(jnp.bfloat16).astype(jnp.float32))
        d_mid = (dy_loc.astype(jnp.float32) + d_mid_norm).astype(jnp.bfloat16)
        d_mid_full = both(d_mid)

        d_attn = dot('tbsd,hd->tbsh', d_mid_full, w_out).astype(jnp.bfloat16)
        d_qkv = attn_bwd(idx, rot, d_attn, cos_t, sin_t, heads)
        dw_out = scatter(dot('tbsh,tbsd->hd', attn, d_mid_full), 1)
        dw_qkv = scatter(dot('tbsd,tbsc->dc', h_attn, d_qkv), 0)
        dha_other = partner(dot('bsc,dc->bsd', d_qkv[1], w_qkv))
        dh_attn = dot('bsc,dc->bsd', d_qkv[0], w_qkv) + dha_other
        d_x_norm, d_gain_attn = norm_back_attn(dh_attn.astype(jnp.bfloat16).astype(jnp.float32))
        dx = (d_mid.astype(jnp.float32) + d_x_norm).astype(jnp.bfloat16)

        y_other = partner(dot('bsf,fd->bsd', gated_act[1], w_down))
        mlp_red = dot('bsf,fd->bsd', gated_act[0], w_down) + y_other
        y_loc = (mid_f32 + mlp_red.astype(jnp.bfloat16).astype(jnp.float32)).astype(jnp.bfloat16)

        gain_grads = lax.psum((d_gain_attn, d_gain_mlp), ('fsdp', 'model'))
        return (y_loc, dx, gain_grads[0], gain_grads[1], dw_qkv, dw_out, dw_gate, dw_up, dw_down)

    in_specs = (act_spec, act_spec, P(), P(), rows_spec, cols_spec, rows_spec, rows_spec, cols_spec, P(), P())
    out_specs = (act_spec, act_spec, P(), P(), rows_spec, cols_spec, rows_spec, rows_spec, cols_spec)

    return jax.shard_map(device_fn, mesh=mesh, in_specs=in_specs, out_specs=out_specs, check_vma=False)
```

```python
import functools

import jax
import jax.numpy as jnp
from jax import lax
from jax.experimental import pallas as pl
from jax.experimental.pallas import tpu as pltpu
from jax.sharding import PartitionSpec as P


NORM_EPS = 1e-5
NEG = -1e30
QB = 256


def rms_scale(x_f32, gain):
    inv_rms = lax.rsqrt(jnp.mean(x_f32 * x_f32, axis=-1, keepdims=True) + NORM_EPS)
    return x_f32 * inv_rms * gain


def nt(a, b):
    return lax.dot_general(a, b, (((1,), (1,)), ((), ())), preferred_element_type=jnp.float32)


def nn(a, b):
    return lax.dot_general(a, b, (((1,), (0,)), ((), ())), preferred_element_type=jnp.float32)


def tn(a, b):
    return lax.dot_general(a, b, (((0,), (0,)), ((), ())), preferred_element_type=jnp.float32)


def causal_mask():
    rows = lax.broadcasted_iota(jnp.int32, (QB, QB), 0)
    cols = lax.broadcasted_iota(jnp.int32, (QB, QB), 1)
    return rows >= cols


def softmax_chunks(q, k_ref, blk, scale, mask):
    lo = blk * QB
    s_diag = jnp.where(mask, nt(q, k_ref[lo:lo + QB, :]) * scale, NEG)
    top = jnp.max(s_diag, axis=-1, keepdims=True)
    if blk:
        s_off = nt(q, k_ref[:lo, :]) * scale
        top = jnp.maximum(top, jnp.max(s_off, axis=-1, keepdims=True))
        e_off = jnp.exp(s_off - top)
        e_diag = jnp.exp(s_diag - top)
        inv = 1.0 / (jnp.sum(e_off, axis=-1, keepdims=True) + jnp.sum(e_diag, axis=-1, keepdims=True))
        return e_off * inv, e_diag * inv
    e_diag = jnp.exp(s_diag - top)
    return None, e_diag * (1.0 / jnp.sum(e_diag, axis=-1, keepdims=True))


def attn_fwd_kernel(heads, seq, dim, idx_ref, qkv_ref, cos_ref, sin_ref, rot_ref, out_ref, k_scr, v_scr):
    half_rows = seq // 2
    first = idx_ref[0]
    where_half = (first, 1 - first)
    mask = causal_mask()
    scale = dim ** -0.5
    kcol, vcol = heads * dim, (heads + 1) * dim
    for half in range(2):
        st = where_half[half]
        rows = slice(half * half_rows, (half + 1) * half_rows)
        key = qkv_ref[st, 0, :, kcol:kcol + dim]
        key = (key * cos_ref[st] + pltpu.roll(key, dim // 2, 1) * sin_ref[st]).astype(jnp.bfloat16)
        val = qkv_ref[st, 0, :, vcol:vcol + dim].astype(jnp.bfloat16)
        k_scr[rows, :] = key
        v_scr[rows, :] = val
        rot_ref[st, 0, :, kcol:kcol + dim] = key
        rot_ref[st, 0, :, vcol:vcol + dim] = val

    @pl.loop(0, heads)
    def _(h):
        col = pl.ds(pl.multiple_of(h * dim, dim), dim)
        for blk in range(seq // QB):
            st = where_half[blk * QB // half_rows]
            r0 = blk * QB % half_rows
            rows = slice(r0, r0 + QB)
            q = qkv_ref[st, 0, rows, col]
            q = (q * cos_ref[st, rows, :] + pltpu.roll(q, dim // 2, 1) * sin_ref[st, rows, :]).astype(jnp.bfloat16)
            rot_ref[st, 0, rows, col] = q
            p_off, p_diag = softmax_chunks(q, k_scr, blk, scale, mask)
            lo = blk * QB
            o = nn(p_diag.astype(jnp.bfloat16), v_scr[lo:lo + QB, :])
            if blk:
                o = o + nn(p_off.astype(jnp.bfloat16), v_scr[:lo, :])
            out_ref[st, 0, rows, col] = o.astype(jnp.bfloat16)


def attn_bwd_kernel(heads, seq, dim, idx_ref, rot_ref, do_ref, cos_ref, sin_ref, dqkv_ref, k_scr, v_scr, dk_scr, dv_scr):
    half_rows = seq // 2
    first = idx_ref[0]
    where_half = (first, 1 - first)
    mask = causal_mask()
    scale = dim ** -0.5
    kcol, vcol = heads * dim, (heads + 1) * dim
    for half in range(2):
        st = where_half[half]
        rows = slice(half * half_rows, (half + 1) * half_rows)
        k_scr[rows, :] = rot_ref[st, 0, :, kcol:kcol + dim]
        v_scr[rows, :] = rot_ref[st, 0, :, vcol:vcol + dim]
    dk_scr[...] = jnp.zeros_like(dk_scr)
    dv_scr[...] = jnp.zeros_like(dv_scr)

    @pl.loop(0, heads)
    def _(h):
        col = pl.ds(pl.multiple_of(h * dim, dim), dim)
        for blk in range(seq // QB):
            st = where_half[blk * QB // half_rows]
            r0 = blk * QB % half_rows
            rows = slice(r0, r0 + QB)
            lo = blk * QB
            q = rot_ref[st, 0, rows, col]
            do = do_ref[st, 0, rows, col]
            p_off, p_diag = softmax_chunks(q, k_scr, blk, scale, mask)
            dp_diag = nt(do, v_scr[lo:lo + QB, :])
            row_dot = jnp.sum(dp_diag * p_diag, axis=-1, keepdims=True)
            if blk:
                dp_off = nt(do, v_scr[:lo, :])
                row_dot = row_dot + jnp.sum(dp_off * p_off, axis=-1, keepdims=True)
            ds_diag = (p_diag * (dp_diag - row_dot) * scale).astype(jnp.bfloat16)
            dq = nn(ds_diag, k_scr[lo:lo + QB, :])
            dk_scr[lo:lo + QB, :] += tn(ds_diag, q)
            dv_scr[lo:lo + QB, :] += tn(p_diag.astype(jnp.bfloat16), do)
            if blk:
                ds_off = (p_off * (dp_off - row_dot) * scale).astype(jnp.bfloat16)
                dq = dq + nn(ds_off, k_scr[:lo, :])
                dk_scr[:lo, :] += tn(ds_off, q)
                dv_scr[:lo, :] += tn(p_off.astype(jnp.bfloat16), do)
            dq = dq * cos_ref[st, rows, :] - pltpu.roll(dq, dim // 2, 1) * sin_ref[st, rows, :]
            dqkv_ref[st, 0, rows, col] = dq.astype(jnp.bfloat16)

    for half in range(2):
        st = where_half[half]
        rows = slice(half * half_rows, (half + 1) * half_rows)
        dk = dk_scr[rows, :]
        dk = dk * cos_ref[st] - pltpu.roll(dk, dim // 2, 1) * sin_ref[st]
        dqkv_ref[st, 0, :, kcol:kcol + dim] = dk.astype(jnp.bfloat16)
        dqkv_ref[st, 0, :, vcol:vcol + dim] = dv_scr[rows, :].astype(jnp.bfloat16)


def blank(shape, dtype):
    return pl.pallas_call(lambda out_ref: None, out_shape=jax.ShapeDtypeStruct(shape, dtype),
                          out_specs=pl.BlockSpec(memory_space=pl.ANY))()


def seq_block(rows, cols):
    return pl.BlockSpec((2, 1, rows, cols), lambda b, idx: (0, b, 0, 0))


def table_block(rows, dim):
    return pl.BlockSpec((2, rows, dim), lambda b, idx: (0, 0, 0))


def attn_fwd(idx, qkv, cos_t, sin_t, heads):
    _, batch, rows, cols = qkv.shape
    dim = cos_t.shape[-1]
    flops = batch * heads * rows * rows * dim * 10
    return pl.pallas_call(
        functools.partial(attn_fwd_kernel, heads, 2 * rows, dim),
        out_shape=(jax.ShapeDtypeStruct(qkv.shape, jnp.bfloat16),
                   jax.ShapeDtypeStruct((2, batch, rows, heads * dim), jnp.bfloat16)),
        grid_spec=pltpu.PrefetchScalarGridSpec(
            num_scalar_prefetch=1, grid=(batch,),
            in_specs=[seq_block(rows, cols), table_block(rows, dim), table_block(rows, dim)],
            out_specs=[seq_block(rows, cols), seq_block(rows, heads * dim)],
            scratch_shapes=[pltpu.VMEM((2 * rows, dim), jnp.bfloat16)] * 2),
        cost_estimate=pl.CostEstimate(flops=flops, bytes_accessed=qkv.size * 8, transcendentals=batch * heads * rows * rows * 2),
        compiler_params=pltpu.CompilerParams(dimension_semantics=("arbitrary",)),
        name="attn_fwd",
    )(idx, qkv, cos_t, sin_t)


def attn_bwd(idx, rot, d_attn, cos_t, sin_t, heads):
    _, batch, rows, cols = rot.shape
    dim = cos_t.shape[-1]
    flops = batch * heads * rows * rows * dim * 25
    return pl.pallas_call(
        functools.partial(attn_bwd_kernel, heads, 2 * rows, dim),
        out_shape=jax.ShapeDtypeStruct(rot.shape, jnp.bfloat16),
        grid_spec=pltpu.PrefetchScalarGridSpec(
            num_scalar_prefetch=1, grid=(batch,),
            in_specs=[seq_block(rows, cols), seq_block(rows, heads * dim), table_block(rows, dim), table_block(rows, dim)],
            out_specs=seq_block(rows, cols),
            scratch_shapes=[pltpu.VMEM((2 * rows, dim), jnp.bfloat16)] * 2 + [pltpu.VMEM((2 * rows, dim), jnp.float32)] * 2),
        cost_estimate=pl.CostEstimate(flops=flops, bytes_accessed=rot.size * 6, transcendentals=batch * heads * rows * rows * 2),
        compiler_params=pltpu.CompilerParams(dimension_semantics=("arbitrary",)),
        name="attn_bwd",
    )(idx, rot, d_attn, cos_t, sin_t)


def solution(mesh):
    act_spec = P('fsdp', 'model', None)
    rows_spec = P('fsdp', 'model')
    cols_spec = P('model', 'fsdp')
    swap = [(0, 1), (1, 0)]

    along_x = [(0, 1), (1, 0), (2, 3), (3, 2)]
    along_y = [(0, 2), (2, 0), (1, 3), (3, 1)]

    def hop(tensor, pairs):
        return lax.ppermute(tensor, 'fsdp', pairs)

    def ring_gather(shard):
        me = lax.axis_index('fsdp')
        rows = shard.shape[0]
        half = rows // 2
        upper, lower = shard[:half], shard[half:]
        y_upper, x_lower = hop(upper, along_y), hop(lower, along_x)
        x_upper, y_lower = hop(upper, along_x), hop(lower, along_y)
        d_upper, d_lower = hop(y_upper, along_x), hop(x_lower, along_y)
        full = jnp.zeros((4 * rows, shard.shape[1]), shard.dtype)
        for offset, parts in ((0, (upper, lower)), (1, (x_upper, x_lower)), (2, (y_upper, y_lower)), (3, (d_upper, d_lower))):
            start = (me ^ offset) * rows
            full = lax.dynamic_update_slice(full, jnp.concatenate(parts), (start, 0))
        return full

    def gather_rows(w_shard):
        return lax.all_gather(w_shard, 'fsdp', axis=0, tiled=True)

    def gather_cols(w_shard):
        return lax.all_gather(w_shard, 'fsdp', axis=1, tiled=True)

    def scatter(tensor, dim):
        return lax.psum_scatter(tensor, 'fsdp', scatter_dimension=dim, tiled=True)

    def partner(tensor):
        return lax.ppermute(tensor, 'model', swap)

    def both(own):
        other = partner(own)
        pair = blank((2,) + own.shape, own.dtype)
        pair = lax.dynamic_update_slice(pair, own[None], (0, 0, 0, 0))
        return lax.dynamic_update_slice(pair, other[None], (1, 0, 0, 0))

    def dot(spec, left, right):
        return jnp.einsum(spec, left, right, preferred_element_type=jnp.float32)

    def device_fn(x_loc, dy_loc, gain_attn, gain_mlp, wqkv_sh, wout_sh, wgate_sh, wup_sh, wdown_sh, rope_cos, rope_sin):
        dim = 2 * rope_cos.shape[1]
        heads = wout_sh.shape[0] // dim
        half_rows = x_loc.shape[1]
        me = lax.axis_index('model')
        idx = jnp.reshape(me, (1,)).astype(jnp.int32)

        def table(first, second):
            full = jnp.concatenate([first, second], axis=-1).reshape(2, half_rows, dim)
            return jnp.where(me == 0, full, full[::-1])

        cos_t = table(rope_cos, rope_cos)
        sin_t = table(-rope_sin, rope_sin)

        w_qkv = ring_gather(wqkv_sh)
        w_gate = gather_rows(wgate_sh)

        x_f32 = x_loc.astype(jnp.float32)
        h_attn_f, norm_back_attn = jax.vjp(rms_scale, x_f32, gain_attn)
        h_own = h_attn_f.astype(jnp.bfloat16)
        h_attn, dy = lax.optimization_barrier((both(h_own), both(dy_loc)))
        qkv = dot('tbsd,dc->tbsc', h_attn, w_qkv)
        wup_sh, qkv = lax.optimization_barrier((wup_sh, qkv))
        w_up = gather_rows(wup_sh)
        w_out_t = ring_gather(wout_sh.T)
        rot, attn = attn_fwd(idx, qkv, cos_t, sin_t, heads)
        wdown_sh, attn = lax.optimization_barrier((wdown_sh, attn))
        w_down = gather_cols(wdown_sh)
        heads_other, w_out_other = partner(attn[1]), partner(w_out_t)
        own_heads = lax.optimization_barrier(dot('bsh,dh->bsd', attn[0], w_out_t))
        attn_red = own_heads + dot('bsh,dh->bsd', heads_other, w_out_other)
        mid_f32 = (x_f32 + attn_red.astype(jnp.bfloat16).astype(jnp.float32)).astype(jnp.bfloat16).astype(jnp.float32)
        h_mlp_f, norm_back_mlp = jax.vjp(rms_scale, mid_f32, gain_mlp)
        h_mlp = both(h_mlp_f.astype(jnp.bfloat16))

        gate = dot('tbsd,df->tbsf', h_mlp, w_gate)
        up_proj = dot('tbsd,df->tbsf', h_mlp, w_up)
        sig_gate = jax.nn.sigmoid(gate)
        silu_gate = gate * sig_gate
        gated_act = (silu_gate * up_proj).astype(jnp.bfloat16)
        full_down, dy = lax.optimization_barrier((dot('tbsf,tbsd->fd', gated_act, dy), dy))
        dw_down = scatter(full_down, 1)

        d_act = dot('tbsd,fd->tbsf', dy, w_down).astype(jnp.bfloat16).astype(jnp.float32)
        d_gate = (d_act * up_proj * sig_gate * (1.0 + gate * (1.0 - sig_gate))).astype(jnp.bfloat16)
        d_up = (d_act * silu_gate).astype(jnp.bfloat16)
        pair = blank((2,) + w_gate.shape, jnp.float32)
        pair = lax.dynamic_update_slice(pair, dot('tbsd,tbsf->df', h_mlp, d_gate)[None], (0, 0, 0))
        pair, h_mlp = lax.optimization_barrier((pair, h_mlp))
        pair = lax.dynamic_update_slice(pair, dot('tbsd,tbsf->df', h_mlp, d_up)[None], (1, 0, 0))
        pair, d_gate, d_up = lax.optimization_barrier((pair, d_gate, d_up))
        dw_gate, dw_up = scatter(pair, 1)

        def dh_of(part):
            return (dot('bsf,df->bsd', d_gate[part], w_gate)
                    + dot('bsf,df->bsd', d_up[part], w_up))

        dh_other = partner(dh_of(1))
        dh_mlp = dh_of(0) + dh_other
        d_mid_norm, d_gain_mlp = norm_back_mlp(dh_mlp.astype(jnp.bfloat16).astype(jnp.float32))
        d_mid = (dy_loc.astype(jnp.float32) + d_mid_norm).astype(jnp.bfloat16)
        d_mid_full = both(d_mid)

        d_attn = dot('tbsd,dh->tbsh', d_mid_full, w_out_t).astype(jnp.bfloat16)
        full_out, d_attn = lax.optimization_barrier((dot('tbsd,tbsh->dh', d_mid_full, attn), d_attn))
        d_qkv = attn_bwd(idx, rot, d_attn, cos_t, sin_t, heads)
        full_qkv = dot('tbsd,tbsc->dc', h_attn, d_qkv)
        both_grads = scatter(jnp.concatenate([full_qkv, full_out], axis=1), 0)
        dw_qkv, dw_out = both_grads[:, :full_qkv.shape[1]], both_grads[:, full_qkv.shape[1]:].T
        dha_other = partner(dot('bsc,dc->bsd', d_qkv[1], w_qkv))
        dh_attn = dot('bsc,dc->bsd', d_qkv[0], w_qkv) + dha_other
        d_x_norm, d_gain_attn = norm_back_attn(dh_attn.astype(jnp.bfloat16).astype(jnp.float32))
        dx = (d_mid.astype(jnp.float32) + d_x_norm).astype(jnp.bfloat16)

        y_other = partner(dot('bsf,fd->bsd', gated_act[1], w_down))
        mlp_red = dot('bsf,fd->bsd', gated_act[0], w_down) + y_other
        y_loc = (mid_f32 + mlp_red.astype(jnp.bfloat16).astype(jnp.float32)).astype(jnp.bfloat16)

        gain_grads = lax.psum((d_gain_attn, d_gain_mlp), ('fsdp', 'model'))
        return (y_loc, dx, gain_grads[0], gain_grads[1], dw_qkv, dw_out, dw_gate, dw_up, dw_down)

    in_specs = (act_spec, act_spec, P(), P(), rows_spec, cols_spec, rows_spec, rows_spec, cols_spec, P(), P())
    out_specs = (act_spec, act_spec, P(), P(), rows_spec, cols_spec, rows_spec, rows_spec, cols_spec)

    return jax.shard_map(device_fn, mesh=mesh, in_specs=in_specs, out_specs=out_specs, check_vma=False)
```
